256 devices in a mesh: dp: 32 (over x, y, z_hi), mp: 8 (over z_lo, core).
Axes of the slice: x: 4, y: 4, z: 8 (z_hi: 2, z_lo: 4; z = z_hi * 4 + z_lo), core: 2. Of those that a mesh axis runs over, the one named last changes fastest.
Arguments:
- tokens: bfloat16 [1024, 7168], P('dp', 'mp'), may hold values from -6 to 6
- gate_weight: bfloat16 [7168, 18432], P('mp', 'dp'), may hold values from -0.0625 to 0.0625
- up_weight: bfloat16 [7168, 18432], P('mp', 'dp'), may hold values from -0.0625 to 0.0625
- down_weight: bfloat16 [18432, 7168], P('dp', 'mp'), may hold values from -0.046875 to 0.046875
- gate_round: bfloat16 [7168, 18432], P('mp', 'dp'), may hold values from -8 to 8
- up_round: bfloat16 [7168, 18432], P('mp', 'dp'), may hold values from -8 to 8
- down_round: bfloat16 [18432, 7168], P('dp', 'mp'), may hold values from -8 to 8
- quant_scale: float32 [2, 18432], P(None, 'dp'), may hold values from 0.3 to 3
- quant_bits: int32 [2, 18432], P(None, 'dp'), may hold values from 2 to 4
- quant_zero: int32 [2, 18432], P(None, 'dp'), may hold values from 0 to 2
- down_scale: float32 [7168], P('mp'), may hold values from 0.3 to 3
- down_bits: int32 [7168], P('mp'), may hold values from 2 to 4
- down_zero: int32 [7168], P('mp'), may hold values from 0 to 2
- fisher: float32 [1024], replicated, may hold values from 1 to 300, as said below
Outputs:
- loss_value: float32 [], replicated
- grad_gate: bfloat16 [7168, 18432], P('mp', 'dp')
- grad_up: bfloat16 [7168, 18432], P('mp', 'dp')
- grad_down: bfloat16 [18432, 7168], P('dp', 'mp')
The draws below stay inside these ranges and needn't reach their ends.
Inputs may be any that keep to these rules, and one draw needn't show every extreme that they name: `fisher`: positive weights.
All inputs are finite; a program needn't handle non-finite values.
Results may differ from the reference program's by a relative error of at most 0.0059.
Values may be sent and summed in bfloat16 or wider, within the bound.
No kernel may reach another device: no remote copies, remote signals or barrier semaphores. Data moves between devices by JAX's collectives and lax.ppermute only.
A program may use at most 128 MiB of HBM per device.

```python
import math
import jax
import jax.numpy as jnp

D = 7168
FF = 18432
TOKENS = 1024


def draw_fisher(key, part):
    position = jnp.arange(TOKENS, dtype=jnp.float32) / max(TOKENS - 1, 1)
    growth = math.log(3.0)
    spread = math.log(10.0)
    jitter = jax.random.uniform(key, (TOKENS,), jnp.float32, 0.0, spread)
    return jnp.exp(growth * position + jitter).astype(jnp.float32)


def set_ends(entries, stream_key, smallest, top_value):
    extent = entries.shape
    place = [jax.random.randint(jax.random.fold_in(stream_key, axis), (), 0, extent[axis]) for axis in range(len(extent))]
    entries = entries.at[tuple(place)].set(smallest)
    longest = extent.index(max(extent))
    place[longest] = (place[longest] + 1) % extent[longest]
    return entries.at[tuple(place)].set(top_value)


def block_scale(rng, shape, pieces, least, top_value):
    def one(axis_at, parts):
        steps = jax.random.uniform(jax.random.fold_in(jax.random.fold_in(rng, 6), axis_at), (parts,), jnp.float32, least / len(pieces), top_value / len(pieces))
        return jnp.repeat(jnp.exp(steps), shape[axis_at] // parts).reshape((-1,) + (1,) * (len(shape) - axis_at - 1))

    level = one(*pieces[0])
    for cut in pieces[1:]:
        level = level * one(*cut)
    return level


def centred(key, dims, deviation, limit, pieces=(), kind=jnp.bfloat16):
    gain = block_scale(key, dims, pieces, -0.22, 0.18) if pieces else 1.0
    values = jax.random.normal(key, dims, jnp.float32) * deviation * gain
    return jnp.minimum(jnp.maximum(values, -limit), limit).astype(kind)


def setup_inputs(seed: int = 0) -> dict:
    key_of = jax.random.split(jax.random.key(seed), 15)
    return {
        "tokens": centred(key_of[0], (TOKENS, D), 1.0, 6.0, ((0, 32), (1, 8))),
        "gate_weight": centred(key_of[1], (D, FF), D ** -0.5, 0.0625, ((0, 8), (1, 32))),
        "up_weight": centred(key_of[2], (D, FF), D ** -0.5, 0.0625, ((0, 8), (1, 32))),
        "down_weight": centred(key_of[3], (FF, D), FF ** -0.5, 0.046875, ((0, 32), (1, 8))),
        "gate_round": centred(key_of[4], (D, FF), 2.0, 8.0, ((0, 8), (1, 32))),
        "up_round": centred(key_of[5], (D, FF), 2.0, 8.0, ((0, 8), (1, 32))),
        "down_round": centred(key_of[6], (FF, D), 2.0, 8.0, ((0, 32), (1, 8))),
        "quant_scale": jnp.clip(jnp.exp(math.log(3.0) - 2.3025851 * jax.random.uniform(key_of[7], (2, FF), jnp.float32) ** block_scale(key_of[7], (2, FF), ((1, 32),), -0.2, 0.2)), 0.3, 3.0),
        "quant_bits": set_ends(jax.random.randint(key_of[8], (2, FF), 2, 5), jax.random.fold_in(key_of[8], 1), 2, 4).astype(jnp.int32),
        "quant_zero": set_ends(jax.random.randint(key_of[9], (2, FF), 0, 3), jax.random.fold_in(key_of[9], 1), 0, 2).astype(jnp.int32),
        "down_scale": jnp.clip(jnp.exp(math.log(3.0) - 2.3025851 * jax.random.uniform(key_of[10], (D,), jnp.float32) ** block_scale(key_of[10], (D,), ((0, 8),), -0.2, 0.2)), 0.3, 3.0),
        "down_bits": set_ends(jax.random.randint(key_of[11], (D,), 2, 5), jax.random.fold_in(key_of[11], 1), 2, 4).astype(jnp.int32),
        "down_zero": set_ends(jax.random.randint(key_of[12], (D,), 0, 3), jax.random.fold_in(key_of[12], 1), 0, 2).astype(jnp.int32),
        "fisher": draw_fisher(jax.random.fold_in(key_of[14], 71), 0),
    }


def soft_weight(weight, variable, channel_scale, bit_width, zero_point, fan_in):
    quant_step = channel_scale / jnp.sqrt(jnp.float32(fan_in))
    offset = jnp.clip(1.2 * jax.nn.sigmoid(variable.astype(jnp.float32)) - 0.1, 0.0, 1.0)
    ceiling = (jnp.left_shift(jnp.int32(1), bit_width) - 1).astype(jnp.float32)
    zero_level = zero_point.astype(jnp.float32)
    levels = jnp.clip(weight.astype(jnp.float32) / quant_step + offset - 0.5 + zero_level, 0.0, ceiling)
    return (quant_step * (levels - zero_level)).astype(jnp.bfloat16)

def reference(tokens, gate_weight, up_weight, down_weight, gate_round, up_round, down_round, quant_scale, quant_bits, quant_zero, down_scale, down_bits, down_zero, fisher):
    gate_student = soft_weight(gate_weight, gate_round, quant_scale[0], quant_bits[0], quant_zero[0], D)
    up_student = soft_weight(up_weight, up_round, quant_scale[1], quant_bits[1], quant_zero[1], D)
    down_student = soft_weight(down_weight, down_round, down_scale, down_bits, down_zero, FF)
    gate_teacher = jnp.dot(tokens, gate_weight, preferred_element_type=jnp.float32)
    up_teacher = jnp.dot(tokens, up_weight, preferred_element_type=jnp.float32)
    gate_own = jnp.dot(tokens, gate_student, preferred_element_type=jnp.float32)
    up_own = jnp.dot(tokens, up_student, preferred_element_type=jnp.float32)
    hidden_teacher = (jax.nn.silu(gate_teacher) * up_teacher).astype(jnp.bfloat16)
    hidden_student = (jax.nn.silu(gate_own) * up_own).astype(jnp.bfloat16)
    output_student = jnp.dot(hidden_student, down_student, preferred_element_type=jnp.float32)
    output_teacher = jnp.dot(hidden_teacher, down_weight, preferred_element_type=jnp.float32)
    residual = output_student - output_teacher
    weighted = fisher[:, None] * residual
    loss_value = jnp.sum(weighted * residual) / (TOKENS * D)
    out_grad = (2.0 * weighted).astype(jnp.bfloat16)
    grad_down = jnp.dot(hidden_student.T, out_grad, preferred_element_type=jnp.float32).astype(jnp.bfloat16)
    hidden_grad = jnp.dot(out_grad, down_student.T, preferred_element_type=jnp.float32)
    sigmoid_gate = jax.nn.sigmoid(gate_own)
    gate_grad = (hidden_grad * up_own * sigmoid_gate * (1.0 + gate_own * (1.0 - sigmoid_gate))).astype(jnp.bfloat16)
    up_grad = (hidden_grad * gate_own * sigmoid_gate).astype(jnp.bfloat16)
    grad_gate = jnp.dot(tokens.T, gate_grad, preferred_element_type=jnp.float32).astype(jnp.bfloat16)
    grad_up = jnp.dot(tokens.T, up_grad, preferred_element_type=jnp.float32).astype(jnp.bfloat16)
    return (loss_value, grad_gate, grad_up, grad_down)
```

```python
import jax
import jax.numpy as jnp
from jax import lax
from jax.sharding import Mesh
from jax.sharding import PartitionSpec as P

D = 7168
FF = 18432
X, Y, H, Z, C = "x", "y", "h", "z", "c"
SIZE = {X: 4, Y: 4, H: 2, Z: 4, C: 2}
DP = (X, Y, H)
MP = (Z, C)
CHUNKS = 2
BF = jnp.bfloat16
F32 = jnp.float32


def shifted(value, axis, by):
    n = SIZE[axis]
    return lax.ppermute(value, axis, [((i + by) % n, i) for i in range(n)])


def flipped(value, axis, bit):
    return lax.ppermute(value, axis, [(i, i ^ bit) for i in range(SIZE[axis])])


def x_slot_pairs(slot):
    return [
        (((x + slot + z) % SIZE[X]) * SIZE[Z] + z, x * SIZE[Z] + z)
        for x in range(SIZE[X])
        for z in range(SIZE[Z])
    ]


def x_fetch(value, slot):
    return lax.ppermute(value, (X, Z), x_slot_pairs(slot))


def x_return(value, slot):
    return lax.ppermute(value, (X, Z), [(b, a) for a, b in x_slot_pairs(slot)])


def gather_rows(block, x_first):
    first_core = lax.axis_index(C) == 0
    other = shifted(block, H, 1)
    both = jnp.stack([jnp.where(first_core, block, other), jnp.where(first_core, other, block)])
    if x_first:
        over_x = jnp.stack([x_fetch(both, s) for s in range(4)], axis=1)
        full = jnp.stack([over_x] + [shifted(over_x, Y, k) for k in range(1, 4)], axis=2)
    else:
        over_y = jnp.stack([both] + [shifted(both, Y, k) for k in range(1, 4)], axis=1)
        full = jnp.stack([x_fetch(over_y, s) for s in range(4)], axis=1)
    return full.reshape(-1, block.shape[-1])


def scatter_rows(terms, rows, x_first):
    first_core = lax.axis_index(C) == 0
    full = terms.reshape(2, 4, 4, rows, terms.shape[-1])
    if x_first:
        sent = full.astype(BF)
        over_x = sum(x_return(sent[:, s], s).astype(F32) for s in range(4))
        both = over_x[:, 0] + sum(shifted(over_x[:, k], Y, -k) for k in range(1, 4))
    else:
        sent = full.astype(BF)
        over_y = full[:, :, 0] + sum(
            shifted(sent[:, :, k], Y, -k).astype(F32) for k in range(1, 4)
        )
        both = sum(x_return(over_y[:, s], s) for s in range(4))
    kept = jnp.where(first_core, both[0], both[1])
    given = jnp.where(first_core, both[1], both[0])
    return kept + shifted(given, H, 1)


def reduce_mp(own_half, other_half):
    rows = own_half.shape[0] // 4
    received = shifted(other_half.astype(BF), C, 1).astype(F32)
    summed = (own_half + received).reshape(4, rows, -1)
    sent = summed.astype(BF)
    return summed[0] + sum(shifted(sent[s], Z, -s).astype(F32) for s in range(1, 4))


def gather_mp(own):
    half = jnp.concatenate([own] + [shifted(own, Z, s) for s in range(1, 4)], axis=0)
    return half, shifted(half, C, 1)


def total(value):
    value = jnp.full((8, 128), value, F32)
    for axis, bit in ((C, 1), (Z, 1), (Z, 2), (X, 1), (X, 2), (Y, 1), (Y, 2), (H, 1)):
        value = value + flipped(value, axis, bit)
    return value[0, 0]


def soft_weight(weight, variable, channel_scale, bit_width, zero_point, fan_in):
    quant_step = channel_scale / jnp.sqrt(jnp.float32(fan_in))
    offset = jnp.clip(1.2 * jax.nn.sigmoid(variable.astype(jnp.float32)) - 0.1, 0.0, 1.0)
    ceiling = (jnp.left_shift(jnp.int32(1), bit_width) - 1).astype(jnp.float32)
    zero_level = zero_point.astype(jnp.float32)
    levels = jnp.clip(
        weight.astype(jnp.float32) / quant_step + offset - 0.5 + zero_level, 0.0, ceiling
    )
    return (quant_step * (levels - zero_level)).astype(jnp.bfloat16)


def product(left, right, left_dim, right_dim):
    return lax.dot_general(
        left, right, (((left_dim,), (right_dim,)), ((), ())), preferred_element_type=F32
    )


def shards(
    tokens,
    gate_weight,
    up_weight,
    down_weight,
    gate_round,
    up_round,
    down_round,
    quant_scale,
    quant_bits,
    quant_zero,
    down_scale,
    down_bits,
    down_zero,
    fisher,
):
    own_rows = tokens.shape[0]
    hidden = gate_weight.shape[1]
    total_rows = fisher.shape[0]
    rows = own_rows // CHUNKS
    order = [k % 2 == 0 for k in range(CHUNKS)]
    token_weight = lax.dynamic_slice_in_dim(fisher, lax.axis_index(DP) * own_rows, own_rows)

    all_tokens = [gather_rows(tokens[k * rows : (k + 1) * rows], order[k]) for k in range(CHUNKS)]

    gate_student = soft_weight(
        gate_weight, gate_round, quant_scale[0], quant_bits[0], quant_zero[0], D
    )
    up_student = soft_weight(up_weight, up_round, quant_scale[1], quant_bits[1], quant_zero[1], D)
    down_student = soft_weight(down_weight, down_round, down_scale, down_bits, down_zero, FF)
    first = lax.optimization_barrier(
        jnp.concatenate([gate_weight.T, gate_student.T, up_weight.T, up_student.T], axis=0)
    )
    second = lax.optimization_barrier(jnp.concatenate([-down_weight, down_student], axis=0))

    gate_up = []
    activations = []
    for k in range(CHUNKS):
        half = all_tokens[k].shape[0] // 2
        other = product(all_tokens[k][half:], first, 1, 1)
        own = product(all_tokens[k][:half], first, 1, 1)
        shares = reduce_mp(own, other)
        gate_up.append(shares)
        both = (jax.nn.silu(shares[:, : 2 * hidden]) * shares[:, 2 * hidden :]).astype(BF)
        activations.append(jnp.concatenate(gather_mp(both), axis=0))

    out_grads = []
    partial_loss = 0.0
    for k in range(CHUNKS):
        terms = product(activations[k], second, 1, 0)
        residual = scatter_rows(terms, rows, order[k])
        weighted = token_weight[k * rows : (k + 1) * rows, None] * residual
        partial_loss = partial_loss + jnp.sum(weighted * residual)
        out_grads.append(gather_rows((2.0 * weighted).astype(BF), order[k]))
    loss_value = total(partial_loss) / (total_rows * D)

    both_grads = []
    for k in range(CHUNKS):
        half = out_grads[k].shape[0] // 2
        other = product(out_grads[k][half:], down_student, 1, 1)
        own = product(out_grads[k][:half], down_student, 1, 1)
        hidden_grad = reduce_mp(own, other)
        gate_own = gate_up[k][:, hidden : 2 * hidden]
        up_own = gate_up[k][:, 3 * hidden :]
        sig = jax.nn.sigmoid(gate_own)
        gate_grad = (hidden_grad * up_own * sig * (1.0 + gate_own * (1.0 - sig))).astype(BF)
        up_grad = (hidden_grad * gate_own * sig).astype(BF)
        mine = jnp.concatenate([gate_grad, up_grad], axis=1)
        both_grads.append(jnp.concatenate(gather_mp(mine), axis=0))

    grad_down = sum(
        product(activations[k][:, hidden:], out_grads[k], 0, 0) for k in range(CHUNKS)
    ).astype(BF)
    weight_grads = sum(product(both_grads[k], all_tokens[k], 0, 0) for k in range(CHUNKS)).astype(
        BF
    )
    return (loss_value, weight_grads[:hidden].T, weight_grads[hidden:].T, grad_down)


def solution(mesh):
    split = Mesh(mesh.devices.reshape(4, 4, 2, 4, 2), (X, Y, H, Z, C))
    return jax.shard_map(
        shards,
        mesh=split,
        in_specs=(
            P(DP, MP),
            P(MP, DP),
            P(MP, DP),
            P(DP, MP),
            P(MP, DP),
            P(MP, DP),
            P(DP, MP),
            P(None, DP),
            P(None, DP),
            P(None, DP),
            P(MP),
            P(MP),
            P(MP),
            P(),
        ),
        out_specs=(P(), P(MP, DP), P(MP, DP), P(DP, MP)),
        check_vma=False,
    )
```

```python
import jax
import jax.numpy as jnp
import numpy as np
from jax import lax
from jax.sharding import Mesh
from jax.sharding import PartitionSpec as P


D = 7168
FF = 18432
X, Y, H, Z, C = "x", "y", "h", "z", "c"
SIZE = {X: 4, Y: 4, H: 2, Z: 4, C: 2}
SLOTS = (0, 2, 1, 3)
DP = (X, Y, H)
MP = (Z, C)
BF = jnp.bfloat16
F32 = jnp.float32


def product(left, right, left_dim, right_dim):
    return lax.dot_general(
        left, right, (((left_dim,), (right_dim,)), ((), ())), preferred_element_type=F32
    )


def flipped(value, axis, bit):
    return lax.ppermute(value, axis, [(i, i ^ bit) for i in range(SIZE[axis])])


def plane_groups():
    place = np.arange(256).reshape(4, 4, 2, 4, 2)
    return [
        [
            int(place[slot ^ z, 2 * (half ^ c) + low, h, z, c])
            for half in range(2)
            for slot in SLOTS
            for low in range(2)
        ]
        for h in range(2)
        for z in range(4)
        for c in range(2)
    ]


def exchange(blocks):
    return lax.all_to_all(
        blocks, (X, Y, H, Z, C), 0, 0, axis_index_groups=plane_groups(), tiled=True
    )


def copied(block):
    return jnp.broadcast_to(block, (16, *block.shape))


def gather_plane(block):
    return exchange(copied(block)).reshape(-1, block.shape[-1])


def scatter_plane(terms):
    blocks = terms.astype(BF).reshape(16, -1, terms.shape[-1])
    return jnp.sum(exchange(blocks).astype(F32), axis=0)


def halves_swapped(value):
    rows = value.shape[0] // 2
    return jnp.concatenate([value[rows:], value[:rows]], axis=0)


def slot_order(per_row):
    z, c = lax.axis_index(Z), lax.axis_index(C)
    table = per_row.reshape(2, 2, 2, 2, 2, -1)
    table = jnp.where(z & 1 == 1, table[:, ::-1], table)
    table = jnp.where(z & 2 == 2, table[::-1], table)
    table = jnp.where(c == 1, table[:, :, ::-1], table)
    table = jnp.where(lax.axis_index(H) == 1, table[:, :, :, :, ::-1], table)
    return table.transpose(2, 1, 0, 3, 4, 5).reshape(-1)


def together(value, *others):
    return lax.optimization_barrier((value, *others))


def joined(first, second):
    return jnp.concatenate([first, second], axis=0)


def added(value, axis, bit):
    return value + flipped(value, axis, bit)


def gathered_half(own):
    pair = joined(own, flipped(own, Z, 2))
    return joined(pair, flipped(pair, Z, 1))


def merged(first, second):
    shape = (-1, 32, first.shape[-1])
    both = jnp.stack([first.reshape(shape), second.reshape(shape)], axis=1)
    return both.reshape(-1, first.shape[-1])


def beside(first, second):
    return jnp.concatenate([first, second], axis=1)


def soft_weight(weight, variable, channel_scale, bit_width, zero_point, fan_in):
    quant_step = channel_scale / jnp.sqrt(jnp.float32(fan_in))
    offset = jnp.clip(1.2 * jax.nn.sigmoid(variable.astype(jnp.float32)) - 0.1, 0.0, 1.0)
    ceiling = (jnp.left_shift(jnp.int32(1), bit_width) - 1).astype(jnp.float32)
    zero_level = zero_point.astype(jnp.float32)
    levels = jnp.clip(
        weight.astype(jnp.float32) / quant_step + offset - 0.5 + zero_level, 0.0, ceiling
    )
    return (quant_step * (levels - zero_level)).astype(jnp.bfloat16)


def shards(
    tokens,
    gate_weight,
    up_weight,
    down_weight,
    gate_round,
    up_round,
    down_round,
    quant_scale,
    quant_bits,
    quant_zero,
    down_scale,
    down_bits,
    down_zero,
    fisher,
):
    hidden = gate_weight.shape[1]
    total_rows = fisher.shape[0]
    own_rows = tokens.shape[0]

    copies = copied(tokens)
    partner = flipped(tokens, H, 1)
    spread = exchange(copies)
    planes = [spread.reshape(-1, tokens.shape[-1]), None]
    (
        partner,
        copies,
        gate_weight,
        up_weight,
        gate_round,
        up_round,
        quant_scale,
        quant_bits,
        quant_zero,
    ) = together(
        partner,
        copies,
        gate_weight,
        up_weight,
        gate_round,
        up_round,
        quant_scale,
        quant_bits,
        quant_zero,
    )
    copies = copied(partner)
    spread = exchange(copies)
    planes[1] = spread.reshape(-1, tokens.shape[-1])

    gate_student = soft_weight(
        gate_weight, gate_round, quant_scale[0], quant_bits[0], quant_zero[0], D
    )
    up_student = soft_weight(up_weight, up_round, quant_scale[1], quant_bits[1], quant_zero[1], D)
    gates, ups = together(
        joined(gate_weight.T, gate_student.T), joined(up_weight.T, up_student.T)
    )
    row_weight = lax.dynamic_slice_in_dim(fisher, lax.axis_index((X, Y)) * 2 * own_rows, 2 * own_rows)
    row_weight = jnp.where(lax.axis_index(H) == 1, halves_swapped(row_weight), row_weight)
    slot_weight = slot_order(fisher)

    shares = []
    near_planes = []
    for k in range(2):
        half = planes[k].shape[0] // 2
        rows = half // 4
        full = [product(planes[k], weight, 1, 1) for weight in (gates, ups)]
        other = flipped(jnp.stack([part[half:].astype(BF) for part in full]), C, 1)
        own = jnp.stack([part[:half] for part in full]) + other
        given = own[:, 2 * rows :].astype(BF)
        if k == 0:
            planes[1], _ = together(planes[1], given)
        kept = own[:, : 2 * rows] + flipped(given, Z, 1)
        share = kept[:, :rows] + flipped(kept[:, rows:].astype(BF), Z, 2)
        shares.append(share)
        both = (jax.nn.silu(share[0]) * share[1]).astype(BF)
        near_planes.append(gathered_half(both))
    near = merged(*near_planes)
    far = flipped(near, C, 1)

    down_weight, down_round, _ = together(down_weight, down_round, shares[0])
    down_student = soft_weight(down_weight, down_round, down_scale, down_bits, down_zero, FF)
    downs, down_student = together(joined(-down_weight, down_student), down_student)

    all_tokens = merged(*planes)
    gate_own = merged(shares[0][0], shares[1][0])[:, hidden:]
    up_own = merged(shares[0][1], shares[1][1])[:, hidden:]
    sig = jax.nn.sigmoid(gate_own)
    factors = joined(
        (up_own * sig * (1.0 + gate_own * (1.0 - sig))).astype(BF).T,
        (gate_own * sig).astype(BF).T,
    )
    factors, _ = together(factors, far)

    terms = joined(
        product(near, downs, 1, 0).astype(BF), product(far, downs, 1, 0).astype(BF)
    )
    partial, received, all_tokens = together(
        scatter_plane(terms).astype(BF), flipped(factors, Z, 2), all_tokens
    )
    pair = beside(factors, received)
    residual = partial.astype(F32) + halves_swapped(flipped(partial, H, 1)).astype(F32)
    pair_grad = (2.0 * (row_weight[:, None] * residual)).astype(BF)
    out_grad, received = together(gather_plane(pair_grad), flipped(pair, Z, 1))
    near_factors = beside(pair, received)

    half = total_rows // 2
    rows = half // 4
    full = product(down_student, out_grad, 1, 1)
    other = flipped(full[:, half:].astype(BF), C, 1)
    given = (full[:, 2 * rows : half] + other[:, 2 * rows :]).astype(BF)
    kept = full[:, : 2 * rows] + other[:, : 2 * rows]
    wide, _ = together(out_grad, given)
    wide = wide.astype(F32)
    loss = jnp.full((8, 128), jnp.sum(wide * wide * (0.25 / slot_weight)[:, None]), F32)
    received, loss, far_factors = together(
        flipped(given, Z, 1), added(loss, C, 1), flipped(near_factors, C, 1)
    )
    kept = kept + received
    received, loss, near_down = together(
        flipped(kept[:, rows:].astype(BF), Z, 2),
        added(loss, Z, 1),
        product(near[:, hidden:], out_grad[:half], 0, 0),
    )
    own = (kept[:, :rows] + received).astype(BF)
    received, loss, grad_down = together(
        flipped(own, Z, 2),
        added(loss, Z, 2),
        (near_down + product(far[:, hidden:], out_grad[half:], 0, 0)).astype(BF),
    )
    pair = beside(own, received)
    near_grad = beside(pair, flipped(pair, Z, 1))
    far_grad = flipped(near_grad, C, 1)

    def weight_grad(first):
        def part(grad, factor, rows):
            scaled = grad.astype(F32) * factor[first : first + hidden]
            return product(scaled.astype(BF), rows, 1, 0)

        return part(near_grad, near_factors, all_tokens[:half]), lambda: part(
            far_grad, far_factors, all_tokens[half:]
        )

    gate_part, gate_rest = weight_grad(0)
    up_part, up_rest = weight_grad(hidden)
    far_grad, gate_part, up_part = together(far_grad, gate_part, up_part)
    grad_gate = (gate_part + gate_rest()).astype(BF)
    grad_up = (up_part + up_rest()).astype(BF)
    loss_value = loss[0, 0] / (total_rows * D)
    return (loss_value, grad_gate.T, grad_up.T, grad_down)


def solution(mesh):
    split = Mesh(mesh.devices.reshape(4, 4, 2, 4, 2), (X, Y, H, Z, C))
    return jax.shard_map(
        shards,
        mesh=split,
        in_specs=(
            P(DP, MP),
            P(MP, DP),
            P(MP, DP),
            P(DP, MP),
            P(MP, DP),
            P(MP, DP),
            P(DP, MP),
            P(None, DP),
            P(None, DP),
            P(None, DP),
            P(MP),
            P(MP),
            P(MP),
            P(),
        ),
        out_specs=(P(), P(MP, DP), P(MP, DP), P(DP, MP)),
        check_vma=False,
    )
```

```python
import jax
import jax.numpy as jnp
import numpy as np
from jax import lax
from jax.sharding import Mesh
from jax.sharding import PartitionSpec as P


D = 7168
FF = 18432
X, Y, H, Z, C = "x", "y", "h", "z", "c"
SIZE = {X: 4, Y: 4, H: 2, Z: 4, C: 2}
SLOTS = (0, 2, 1, 3)
DP = (X, Y, H)
MP = (Z, C)
BF = jnp.bfloat16
F32 = jnp.float32


def product(left, right, left_dim, right_dim):
    return lax.dot_general(
        left, right, (((left_dim,), (right_dim,)), ((), ())), preferred_element_type=F32
    )


def flipped(value, axis, bit):
    return lax.ppermute(value, axis, [(i, i ^ bit) for i in range(SIZE[axis])])


def plane_groups():
    place = np.arange(256).reshape(4, 4, 2, 4, 2)
    return [
        [
            int(place[slot ^ z, 2 * (half ^ c) + low, h, z, c])
            for half in range(2)
            for slot in SLOTS
            for low in range(2)
        ]
        for h in range(2)
        for z in range(4)
        for c in range(2)
    ]


def exchange(blocks):
    return lax.all_to_all(
        blocks, (X, Y, H, Z, C), 0, 0, axis_index_groups=plane_groups(), tiled=True
    )


def copied(block):
    return jnp.broadcast_to(block, (16, *block.shape))


def gather_plane(block):
    return exchange(copied(block)).reshape(-1, block.shape[-1])


def scatter_plane(terms):
    blocks = terms.astype(BF).reshape(16, -1, terms.shape[-1])
    return jnp.sum(exchange(blocks).astype(F32), axis=0)


def halves_swapped(value):
    rows = value.shape[0] // 2
    return jnp.concatenate([value[rows:], value[:rows]], axis=0)


def slot_order(per_row):
    z, c = lax.axis_index(Z), lax.axis_index(C)
    table = per_row.reshape(2, 2, 2, 2, 2, -1)
    table = jnp.where(z & 1 == 1, table[:, ::-1], table)
    table = jnp.where(z & 2 == 2, table[::-1], table)
    table = jnp.where(c == 1, table[:, :, ::-1], table)
    table = jnp.where(lax.axis_index(H) == 1, table[:, :, :, :, ::-1], table)
    return table.transpose(2, 1, 0, 3, 4, 5).reshape(-1)


def together(value, *others):
    return lax.optimization_barrier((value, *others))


def joined(first, second):
    return jnp.concatenate([first, second], axis=0)


def added(value, axis, bit):
    return value + flipped(value, axis, bit)


def merged(first, second):
    shape = (-1, 32, first.shape[-1])
    both = jnp.stack([first.reshape(shape), second.reshape(shape)], axis=1)
    return both.reshape(-1, first.shape[-1])


def beside(first, second):
    return jnp.concatenate([first, second], axis=1)


def soft_weight(weight, variable, channel_scale, bit_width, zero_point, fan_in):
    quant_step = channel_scale / jnp.sqrt(jnp.float32(fan_in))
    offset = jnp.clip(1.2 * jax.nn.sigmoid(variable.astype(jnp.float32)) - 0.1, 0.0, 1.0)
    ceiling = (jnp.left_shift(jnp.int32(1), bit_width) - 1).astype(jnp.float32)
    zero_level = zero_point.astype(jnp.float32)
    levels = jnp.clip(
        weight.astype(jnp.float32) / quant_step + offset - 0.5 + zero_level, 0.0, ceiling
    )
    return (quant_step * (levels - zero_level)).astype(jnp.bfloat16)


def shards(
    tokens,
    gate_weight,
    up_weight,
    down_weight,
    gate_round,
    up_round,
    down_round,
    quant_scale,
    quant_bits,
    quant_zero,
    down_scale,
    down_bits,
    down_zero,
    fisher,
):
    hidden = gate_weight.shape[1]
    total_rows = fisher.shape[0]
    own_rows = tokens.shape[0]

    copies = copied(tokens)
    partner = flipped(tokens, H, 1)
    spread = exchange(copies)
    planes = [spread.reshape(-1, tokens.shape[-1]), None]
    (
        partner,
        copies,
        gate_weight,
        up_weight,
        gate_round,
        up_round,
        quant_scale,
        quant_bits,
        quant_zero,
    ) = together(
        partner,
        copies,
        gate_weight,
        up_weight,
        gate_round,
        up_round,
        quant_scale,
        quant_bits,
        quant_zero,
    )
    copies = copied(partner)
    spread = exchange(copies)
    planes[1] = spread.reshape(-1, tokens.shape[-1])

    gate_student = soft_weight(
        gate_weight, gate_round, quant_scale[0], quant_bits[0], quant_zero[0], D
    )
    up_student = soft_weight(up_weight, up_round, quant_scale[1], quant_bits[1], quant_zero[1], D)
    gates, ups = together(
        joined(gate_weight.T, gate_student.T), joined(up_weight.T, up_student.T)
    )
    row_weight = lax.dynamic_slice_in_dim(fisher, lax.axis_index((X, Y)) * 2 * own_rows, 2 * own_rows)
    row_weight = jnp.where(lax.axis_index(H) == 1, halves_swapped(row_weight), row_weight)
    slot_weight = slot_order(fisher)

    shares = []
    near_planes = []
    for k in range(2):
        half = planes[k].shape[0] // 2
        rows = half // 4
        full = [product(planes[k], weight, 1, 1) for weight in (gates, ups)]
        other = flipped(jnp.stack([part[half:].astype(BF) for part in full]), C, 1)
        own = jnp.stack([part[:half] for part in full]) + other
        given = own[:, 2 * rows :].astype(BF)
        if k == 0:
            planes[1], _ = together(planes[1], given)
        received = flipped(given, Z, 1)
        kept = own[:, : 2 * rows] + received
        received = flipped(kept[:, rows:].astype(BF), Z, 2)
        share = kept[:, :rows] + received
        shares.append(share)
        both = (jax.nn.silu(share[0]) * share[1]).astype(BF)
        received = flipped(both, Z, 2)
        pair = joined(both, received)
        received = flipped(pair, Z, 1)
        near_planes.append(joined(pair, received))
    near = merged(*near_planes)
    far = flipped(near, C, 1)

    down_weight, down_round, _ = together(down_weight, down_round, shares[0])
    down_student = soft_weight(down_weight, down_round, down_scale, down_bits, down_zero, FF)
    downs, down_student = together(joined(-down_weight, down_student), down_student)

    all_tokens = merged(*planes)
    gate_own = merged(shares[0][0], shares[1][0])[:, hidden:]
    up_own = merged(shares[0][1], shares[1][1])[:, hidden:]
    sig = jax.nn.sigmoid(gate_own)
    factors = joined(
        (up_own * sig * (1.0 + gate_own * (1.0 - sig))).astype(BF).T,
        (gate_own * sig).astype(BF).T,
    )
    factors, _ = together(factors, far)

    terms = joined(
        product(near, downs, 1, 0).astype(BF), product(far, downs, 1, 0).astype(BF)
    )
    partial, received = together(scatter_plane(terms).astype(BF), flipped(factors, Z, 2))
    pair = beside(factors, received)
    residual = partial.astype(F32) + halves_swapped(flipped(partial, H, 1)).astype(F32)
    pair_grad = (2.0 * (row_weight[:, None] * residual)).astype(BF)
    out_grad, received = together(gather_plane(pair_grad), flipped(pair, Z, 1))
    near_factors = beside(pair, received)

    half = total_rows // 2
    rows = half // 4
    full = product(down_student, out_grad, 1, 1)
    other = flipped(full[:, half:].astype(BF), C, 1)
    given = (full[:, 2 * rows : half] + other[:, 2 * rows :]).astype(BF)
    kept = full[:, : 2 * rows] + other[:, : 2 * rows]
    wide, _ = together(out_grad, given)
    wide = wide.astype(F32)
    loss = jnp.full((8, 128), jnp.sum(wide * wide * (0.25 / slot_weight)[:, None]), F32)
    received, loss, far_factors = together(
        flipped(given, Z, 1), added(loss, C, 1), flipped(near_factors, C, 1)
    )
    kept = kept + received
    received, loss, near_down = together(
        flipped(kept[:, rows:].astype(BF), Z, 2),
        added(loss, Z, 1),
        product(near[:, hidden:], out_grad[:half], 0, 0),
    )
    own = (kept[:, :rows] + received).astype(BF)
    received, loss, grad_down, near_gate, near_up = together(
        flipped(own, Z, 2),
        added(loss, Z, 2),
        (near_down + product(far[:, hidden:], out_grad[half:], 0, 0)).astype(BF),
        near_factors[:hidden],
        near_factors[hidden:],
    )
    pair = beside(own, received)
    received, far_gate, far_up = together(
        flipped(pair, Z, 1), far_factors[:hidden], far_factors[hidden:]
    )
    near_grad = beside(pair, received)
    far_grad = flipped(near_grad, C, 1)

    def weight_part(grad, factor, rows):
        return product((grad.astype(F32) * factor).astype(BF), rows, 1, 0)

    near_tokens, far_tokens = all_tokens[:half], all_tokens[half:]
    far_grad, gate_part, up_part = together(
        far_grad,
        weight_part(near_grad, near_gate, near_tokens),
        weight_part(near_grad, near_up, near_tokens),
    )
    gate_rest = weight_part(far_grad, far_gate, far_tokens)
    up_rest = weight_part(far_grad, far_up, far_tokens)
    grad_gate = (gate_part + gate_rest).astype(BF)
    grad_up = (up_part + up_rest).astype(BF)
    loss_value = loss[0, 0] / (total_rows * D)
    return (loss_value, grad_gate.T, grad_up.T, grad_down)


def solution(mesh):
    split = Mesh(mesh.devices.reshape(4, 4, 2, 4, 2), (X, Y, H, Z, C))
    return jax.shard_map(
        shards,
        mesh=split,
        in_specs=(
            P(DP, MP),
            P(MP, DP),
            P(MP, DP),
            P(DP, MP),
            P(MP, DP),
            P(MP, DP),
            P(DP, MP),
            P(None, DP),
            P(None, DP),
            P(None, DP),
            P(MP),
            P(MP),
            P(MP),
            P(),
        ),
        out_specs=(P(), P(MP, DP), P(MP, DP), P(DP, MP)),
        check_vma=False,
    )
```
